32 devices in a mesh: rows: 8 (over z, y), cols: 4 (over x, core).
Axes of the slice: x: 2, y: 2, z: 4, core: 2. Of those that a mesh axis runs over, the one named last changes fastest.
Arguments:
- projector_matrix: float32 [8192, 4096], P('rows', 'cols'), may hold values from -0.0625 to 0.0625
- start_state: float32 [128, 4096], P(None, 'cols'), may hold values from -6 to 6
- decay_rate: float32 [4096], P('cols'), may hold values from 0.05 to 0.95
- escape_heat_factor: float32 [8192], P('rows'), may hold values from 0.1 to 1
- tile_block: int32 [64], P('rows'), may hold values from 0 to 63, as said below
- block_owner: int32 [64], replicated, may hold values from 0 to 7, as said below
- owner_power: float32 [4, 128, 64], P(None, None, 'rows'), may hold values from 0.2 to 5
Outputs:
- final_state: float32 [128, 4096], P(None, 'cols')
- node_temps: float32 [128, 8192], P('cols', 'rows')
- block_history: float32 [4, 128, 64], P(None, 'cols', 'rows')
The draws below stay inside these ranges and needn't reach their ends.
Inputs may be any that keep to these rules, and one draw needn't show every extreme that they name: `block_owner`: every rows index owns exactly 8 blocks. `tile_block`: each block is named by exactly one tile.
All inputs are finite; a program needn't handle non-finite values.
Results may differ from the reference program's by a relative error of at most 0.0001.
Values sent between devices are 32-bit elements; how exact they have to be, the bound alone decides.
A program may use at most 64 MiB of HBM per device.

```python
import math
import jax
import jax.numpy as jnp
from jax import lax

Q = 4096
HEAT_SCENES = 128
STEPS = 4
PATCH_POINTS = 128
MESH_POINTS = 8192
PATCH_TOTAL = 64
BLOCKS = 64
BLK_DEV = 8
N_ROWS = 8


def joint_floorplan(key):
    owner_key = jax.random.fold_in(key, 11)
    offset_key = jax.random.fold_in(key, 23)
    slot_key = jax.random.fold_in(key, 37)
    shuffled = jax.random.permutation(owner_key, jnp.arange(BLOCKS, dtype=jnp.int32))
    owners = (shuffled // BLK_DEV).astype(jnp.int32)
    grouped = jnp.argsort(owners, stable=True).astype(jnp.int32)
    half_rows = N_ROWS // 2
    offsets = jax.random.randint(offset_key, (BLK_DEV,), 0, half_rows, dtype=jnp.int32) * 2
    slots_all = jnp.arange(BLK_DEV, dtype=jnp.int32)
    offsets = (offsets + jnp.where(slots_all == 0, 1, 0)).astype(jnp.int32)
    tiles = jnp.arange(PATCH_TOTAL, dtype=jnp.int32)
    holder = tiles // BLK_DEV
    slot = tiles % BLK_DEV
    target = (3 * holder + offsets[slot]) % N_ROWS
    rotate = jax.random.randint(slot_key, (N_ROWS,), 0, BLK_DEV, dtype=jnp.int32)
    place = (slot + rotate[target]) % BLK_DEV
    picked = grouped[target * BLK_DEV + place]
    return (owners, picked.astype(jnp.int32))


def draw_block_owner(key, part):
    owners, picked = joint_floorplan(key)
    return owners


def draw_tile_block(key, part):
    owners, picked = joint_floorplan(key)
    return picked


def shard_levels(rng, dims, split, least, high):
    factor_of, own = 1.0, jax.random.fold_in(rng, 6)
    for dim, shards_of in split:
        steps = jnp.exp(jax.random.uniform(jax.random.fold_in(own, dim), (shards_of,), jnp.float32, least / len(split), high / len(split)))
        factor_of = factor_of * jnp.repeat(steps, dims[dim] // shards_of).reshape([-1 if axis == dim else 1 for axis in range(len(dims))])
    return factor_of


def gaussian(own_key, shape, width, most, split=(), kind=jnp.bfloat16):
    drawn = jax.random.normal(own_key, shape, jnp.float32) * width
    if len(split) > 0:
        drawn = shard_levels(own_key, shape, split, -0.22, 0.18) * drawn
    return jnp.clip(drawn, min=-most, max=most).astype(kind)


def setup_inputs(seed: int = 0) -> dict:
    splits = jax.random.split(jax.random.key(seed), 8)
    projector_matrix = gaussian(splits[0], (MESH_POINTS, Q), MESH_POINTS ** -0.5, 0.0625, ((0, 8), (1, 4)), jnp.float32)
    start_state = gaussian(splits[1], (HEAT_SCENES, Q), 1.0, 6.0, ((1, 4),), jnp.float32)
    decay_rate = jnp.clip(jnp.exp(math.log(0.95) - 2.944439 * jax.random.uniform(splits[2], (Q,), jnp.float32) ** shard_levels(splits[2], (Q,), ((0, 4),), -0.2, 0.2)), 0.05, 0.95)
    escape_heat_factor = jnp.clip(jnp.exp(math.log(1.0) - 2.3025851 * jax.random.uniform(splits[3], (MESH_POINTS,), jnp.float32) ** shard_levels(splits[3], (MESH_POINTS,), ((0, 8),), -0.2, 0.2)), 0.1, 1.0)
    tile_block = draw_tile_block(jax.random.fold_in(splits[7], 71), 0)
    block_owner = draw_block_owner(jax.random.fold_in(splits[7], 71), 0)
    owner_power = jnp.clip(jnp.exp(math.log(5.0) - 3.218876 * jax.random.uniform(splits[6], (STEPS, HEAT_SCENES, BLOCKS), jnp.float32) ** shard_levels(splits[6], (STEPS, HEAT_SCENES, BLOCKS), ((2, 8),), -0.2, 0.2)), 0.2, 5.0)
    return {"projector_matrix": projector_matrix, "start_state": start_state, "decay_rate": decay_rate, "escape_heat_factor": escape_heat_factor, "tile_block": tile_block, "block_owner": block_owner, "owner_power": owner_power}


escape_heat_derivative = 2.0
dominant_spectral_direction = lax.Precision.HIGHEST


def floor_positions(block_owner, per_owner):
    indices = jnp.arange(block_owner.shape[0], dtype=jnp.int32)
    same_owner = (block_owner[:, None] == block_owner[None, :]) & (indices[None, :] < indices[:, None])
    return block_owner * per_owner + jnp.sum(same_owner.astype(jnp.int32), axis=1)


def reference(projector_matrix, start_state, decay_rate, escape_heat_factor, tile_block, block_owner, owner_power):
    positions = floor_positions(block_owner, BLK_DEV)
    tile_position = positions[tile_block]
    columns = jnp.arange(BLOCKS, dtype=jnp.int32)
    tile_onehot = (tile_position[:, None] == columns[None, :]).astype(jnp.float32)
    compact_vector = start_state
    march_history = []
    point_heat_level = jnp.zeros((HEAT_SCENES, MESH_POINTS), jnp.float32)
    for step_index in range(STEPS):
        point_heat_level = jnp.einsum("ec,wc->ew", compact_vector, projector_matrix, precision=dominant_spectral_direction)
        patch_mean_level = jnp.sum(point_heat_level.reshape(HEAT_SCENES, PATCH_TOTAL, PATCH_POINTS), axis=2) * (1.0 / PATCH_POINTS)
        march_history.append(jnp.dot(patch_mean_level, tile_onehot, precision=dominant_spectral_direction))
        heating_at_patches = jnp.einsum("sb,tb->st", owner_power[step_index], tile_onehot, precision=dominant_spectral_direction)
        heating_at_points = jnp.repeat(heating_at_patches, PATCH_POINTS, axis=1) + escape_heat_factor[None, :] * (1.0 + jnp.tanh(escape_heat_derivative * point_heat_level))
        driven = jnp.dot(heating_at_points, projector_matrix, precision=dominant_spectral_direction)
        compact_vector = decay_rate * compact_vector + (1.0 - decay_rate) * driven
    return compact_vector, point_heat_level, jnp.stack(march_history)
```

```python
import functools

import jax
import jax.numpy as jnp
from jax import lax
from jax.experimental import pallas as pl
from jax.experimental.pallas import tpu as pltpu
from jax.sharding import PartitionSpec as P

STEPS = 4
PATCH_POINTS = 128
GROUPS = 2
LAG = 4
BLOCK = 256
MESH = pl.DeviceIdType.MESH
ORDERS = ((0, 1, 2), (1, 0, 2))


def log2(n):
    return n.bit_length() - 1


def split(x):
    hi = x.astype(jnp.bfloat16)
    return hi, (x - hi.astype(jnp.float32)).astype(jnp.bfloat16)


def dot(a, b, dims):
    return lax.dot_general(a, b, (dims, ((), ())), preferred_element_type=jnp.float32)


NN = ((1,), (0,))
NT = ((1,), (1,))


def kernel(
    n_rows, n_cols, p_ref, start_ref, decay_ref, escape_ref, nodepos_ref, power_ref,
    final_ref, temps_ref, hist_ref,
    p_hi, p_lo, spread, state, lhs, t_part, t_rx, t_full, d_part, d_rx, d_full,
    all_power, power_t, shares, h_part, h_rx, send_sem, recv_sem,
):
    r, q = lax.axis_index("rows"), lax.axis_index("cols")
    kr, kc = log2(n_rows), log2(n_cols)
    scen, states = start_ref.shape
    nodes = p_ref.shape[0]
    size = scen // GROUPS
    tiles = size // 8
    share = scen // n_cols
    positions = spread.shape[0]

    def bit(i, b):
        return (i // (1 << b)) % 2

    def flip(i, b):
        return i + (1 - 2 * bit(i, b)) * (1 << b)

    def row_peer(b):
        return (flip(r, b), q)

    def col_peer(b):
        return (r, flip(q, b))

    barrier = pltpu.get_barrier_semaphore()
    peers = [row_peer(b) for b in range(kr)] + [col_peer(b) for b in range(kc)]
    for peer in peers:
        pl.semaphore_signal(barrier, inc=1, device_id=peer, device_id_type=MESH)

    state[...] = start_ref[...]
    used = [0]
    copies = []

    def send(src, dst, peer):
        slot = used[0]
        used[0] += 1
        copy = pltpu.make_async_remote_copy(
            src_ref=src, dst_ref=dst, send_sem=send_sem.at[slot], recv_sem=recv_sem.at[slot],
            device_id=peer, device_id_type=MESH,
        )
        copy.start()
        copies.append(copy)
        return copy

    @pl.loop(0, nodes // BLOCK)
    def _(i):
        at = pl.ds(pl.multiple_of(i * BLOCK, BLOCK), BLOCK)
        hi, lo = split(p_ref[at, :])
        p_hi[at, :] = hi
        p_lo[at, :] = lo

    rows_iota = lax.broadcasted_iota(jnp.int32, (positions, nodes), 0)
    spread[...] = jnp.where(rows_iota == nodepos_ref[...], 1.0, 0.0).astype(jnp.bfloat16)
    pl.semaphore_wait(barrier, len(peers))

    ready = []

    def power_chain():
        all_power[pl.ds(r, 1)] = power_ref[...][None]
        for b in range(kr):
            block = pl.ds((r // (1 << b)) * (1 << b), 1 << b)
            copy = send(all_power.at[block], all_power.at[block], row_peer(b))
            yield
            copy.wait_recv()
        for k in range(STEPS):
            table = all_power[:, k].reshape(positions, scen).T
            hi, lo = split(table)
            power_t[k, 0] = hi
            power_t[k, 1] = lo
        ready.append(True)

    def history_chain():
        hi, lo = split(shares[...].reshape(STEPS * share, nodes))
        both = dot(spread[...], hi, NT) + dot(spread[...], lo, NT)
        h_part[...] = (both * (1.0 / PATCH_POINTS)).reshape(n_rows, 8, STEPS * share)
        start, length, at = 0, n_rows, 0
        for b in reversed(range(kr)):
            length //= 2
            keep = start + bit(r, b) * length
            away = start + (1 - bit(r, b)) * length
            copy = send(h_part.at[pl.ds(away, length)], h_rx.at[pl.ds(at, length)], row_peer(b))
            yield
            copy.wait_recv()
            kept = pl.ds(keep, length)
            h_part[kept] = h_part[kept] + h_rx[pl.ds(at, length)]
            start, at = keep, at + length
        hist_ref[...] = h_part[pl.ds(r, 1)][0]

    extra = []

    def chain(g):
        mine = slice(g * size, (g + 1) * size)
        width = d_part.shape[-1]
        units = d_part.shape[1] // GROUPS
        unit0 = g * units
        order = ORDERS[g % 2] if kr == 3 else tuple(range(kr))

        def load_lhs():
            for c in range(0, states, BLOCK):
                hi, lo = split(state[mine, c : c + BLOCK])
                lhs[g, :size, c : c + BLOCK] = hi
                lhs[g, size:, c : c + BLOCK] = lo

        load_lhs()
        for k in range(STEPS):

            @pl.loop(0, nodes // BLOCK)
            def _(i):
                at = pl.ds(pl.multiple_of(i * BLOCK, BLOCK), BLOCK)
                two = dot(lhs[g], p_hi[at, :], NT)
                out = two[:size] + two[size:] + dot(lhs[g, :size], p_lo[at, :], NT)
                t_part[k, pl.ds(g * tiles, tiles), :, at] = out.reshape(tiles, 8, BLOCK)

            start, length, at = g * tiles, tiles, g * tiles
            for b in range(kc - 1):
                length //= 2
                keep = start + bit(q, b) * length
                away = start + (1 - bit(q, b)) * length
                copy = send(t_part.at[k, pl.ds(away, length)], t_rx.at[k, pl.ds(at, length)], col_peer(b))
                yield
                copy.wait_recv()
                kept = pl.ds(keep, length)
                t_part[k, kept] = t_part[k, kept] + t_rx[k, pl.ds(at, length)]
                start, at = keep, at + length
            kept = pl.ds(start, length)
            copy = send(t_part.at[k, kept], t_rx.at[k, pl.ds(at, length)], col_peer(kc - 1))
            yield
            copy.wait_recv()
            t_full[k, kept] = t_part[k, kept] + t_rx[k, pl.ds(at, length)]
            for b in reversed(range(kc - 1)):
                kept = pl.ds(start, length)
                copy = send(t_full.at[k, kept], t_full.at[k, kept], col_peer(b))
                yield
                copy.wait_recv()
                start, length = start - bit(q, b) * length, 2 * length

            if g == GROUPS - 1:
                own = t_full[k, pl.ds(q * (share // 8), share // 8)]
                shares[k] = own.reshape(share, nodes)
                if k == STEPS - 1:
                    temps_ref[...] = own.reshape(share, nodes)
                    extra.append(history_chain())

            while not ready:
                yield

            @pl.loop(0, nodes // BLOCK)
            def _(i):
                at = pl.ds(pl.multiple_of(i * BLOCK, BLOCK), BLOCK)
                heat = dot(power_t[k, 0, mine], spread[:, at], NN) + dot(power_t[k, 1, mine], spread[:, at], NN)
                temp = t_full[k, pl.ds(g * tiles, tiles), :, at].reshape(size, BLOCK)
                hi, lo = split(heat + escape_ref[:, at] * (1.0 + jnp.tanh(2.0 * temp)))
                lhs[g, :size, at] = hi
                lhs[g, size:, at] = lo

            @pl.loop(0, states // BLOCK)
            def _(i):
                at = pl.ds(pl.multiple_of(i * BLOCK, BLOCK), BLOCK)
                two = dot(lhs[g], p_hi[:, at], NN)
                out = two[:size] + two[size:] + dot(lhs[g, :size], p_lo[:, at], NN)
                unit = (i * BLOCK) // width
                inner = pl.ds(pl.multiple_of((i * BLOCK) % width, BLOCK), BLOCK)
                d_part[k, pl.ds(unit0 + unit * tiles, tiles), :, inner] = out.reshape(tiles, 8, BLOCK)

            start, length, at = unit0, units, unit0
            for b in order[:-1]:
                length //= 2
                keep = start + bit(r, b) * length
                away = start + (1 - bit(r, b)) * length
                copy = send(d_part.at[k, pl.ds(away, length)], d_rx.at[k, pl.ds(at, length)], row_peer(b))
                yield
                copy.wait_recv()
                kept = pl.ds(keep, length)
                d_part[k, kept] = d_part[k, kept] + d_rx[k, pl.ds(at, length)]
                start, at = keep, at + length
            kept = pl.ds(start, length)
            copy = send(d_part.at[k, kept], d_rx.at[k, pl.ds(at, length)], row_peer(order[-1]))
            yield
            copy.wait_recv()
            d_full[k, kept] = d_part[k, kept] + d_rx[k, pl.ds(at, length)]
            for b in reversed(order[:-1]):
                kept = pl.ds(start, length)
                copy = send(d_full.at[k, kept], d_full.at[k, kept], row_peer(b))
                yield
                copy.wait_recv()
                start, length = start - bit(r, b) * length, 2 * length

            for j in range(states // width):
                cols = slice(j * width, (j + 1) * width)
                keep_share = decay_ref[:, cols]
                driven = d_full[k, unit0 + j * tiles : unit0 + (j + 1) * tiles].reshape(size, width)
                state[mine, cols] = keep_share * state[mine, cols] + (1.0 - keep_share) * driven
            if k < STEPS - 1:
                load_lhs()
            else:
                final_ref[mine, :] = state[mine, :]

    running = [(0, power_chain())] + [(g * LAG, chain(g)) for g in range(GROUPS)]
    tick = 0
    while running or extra:
        running += [(tick, c) for c in extra]
        extra.clear()
        left = []
        for when, c in running:
            if when > tick:
                left.append((when, c))
                continue
            try:
                next(c)
                left.append((when, c))
            except StopIteration:
                pass
        running = left
        tick += 1
    for copy in copies:
        copy.wait_send()


def shards(projector_matrix, start_state, decay_rate, escape_heat_factor, tile_block, block_owner, owner_power):
    n_rows, n_cols = lax.axis_size("rows"), lax.axis_size("cols")
    kr, kc = log2(n_rows), log2(n_cols)
    nodes, states = projector_matrix.shape
    scen = start_state.shape[0]
    share = scen // n_cols
    per_owner = owner_power.shape[2]
    blocks = block_owner.shape[0]
    ids = jnp.arange(blocks, dtype=jnp.int32)
    same = (block_owner[:, None] == block_owner[None, :]) & (ids[None, :] < ids[:, None])
    position = block_owner * per_owner + jnp.sum(same.astype(jnp.int32), axis=1)
    tile_position = jnp.sum(jnp.where(tile_block[:, None] == ids[None, :], position[None, :], 0), axis=1)
    node_position = jnp.repeat(tile_position, PATCH_POINTS)[None, :]
    size = scen // GROUPS
    tiles = size // 8
    need = n_rows // 2
    width = states
    while (tiles * (states // width)) % need:
        width //= 2
    units = GROUPS * tiles * (states // width)
    sems = STEPS * GROUPS * (2 * kr - 1 + 2 * kc - 1) + 2 * kr
    f32, b16 = jnp.float32, jnp.bfloat16
    vmem = pl.BlockSpec(memory_space=pltpu.VMEM)
    final, temps, hist = pl.pallas_call(
        functools.partial(kernel, n_rows, n_cols),
        out_shape=(
            jax.ShapeDtypeStruct((scen, states), f32),
            jax.ShapeDtypeStruct((share, nodes), f32),
            jax.ShapeDtypeStruct((per_owner, STEPS * share), f32),
        ),
        in_specs=[vmem] * 6,
        out_specs=(vmem,) * 3,
        scratch_shapes=[
            pltpu.VMEM((nodes, states), b16),
            pltpu.VMEM((nodes, states), b16),
            pltpu.VMEM((blocks, nodes), b16),
            pltpu.VMEM((scen, states), f32),
            pltpu.VMEM((GROUPS, 2 * size, max(states, nodes)), b16),
            pltpu.VMEM((STEPS, scen // 8, 8, nodes), f32),
            pltpu.VMEM((STEPS, scen // 8, 8, nodes), f32),
            pltpu.VMEM((STEPS, scen // 8, 8, nodes), f32),
            pltpu.VMEM((STEPS, units, 8, width), f32),
            pltpu.VMEM((STEPS, units, 8, width), f32),
            pltpu.VMEM((STEPS, units, 8, width), f32),
            pltpu.VMEM((n_rows, STEPS, per_owner, scen), f32),
            pltpu.VMEM((STEPS, 2, scen, blocks), b16),
            pltpu.VMEM((STEPS, share, nodes), f32),
            pltpu.VMEM((n_rows, per_owner, STEPS * share), f32),
            pltpu.VMEM((n_rows, per_owner, STEPS * share), f32),
            pltpu.SemaphoreType.DMA((sems,)),
            pltpu.SemaphoreType.DMA((sems,)),
        ],
        compiler_params=pltpu.CompilerParams(
            collective_id=0, has_side_effects=True, vmem_limit_bytes=60 * 1024 * 1024
        ),
    )(
        projector_matrix, start_state, decay_rate[None, :], escape_heat_factor[None, :],
        node_position, jnp.transpose(owner_power, (0, 2, 1)),
    )
    history = jnp.transpose(hist.reshape(per_owner, STEPS, share), (1, 2, 0))
    return final, temps, history


def solution(mesh):
    placed = (
        P("rows", "cols"),
        P(None, "cols"),
        P("cols"),
        P("rows"),
        P("rows"),
        P(),
        P(None, None, "rows"),
    )
    return jax.shard_map(
        shards,
        mesh=mesh,
        in_specs=placed,
        out_specs=(P(None, "cols"), P("cols", "rows"), P(None, "cols", "rows")),
        check_vma=False,
    )
```

```python
import functools

import jax
import jax.numpy as jnp
from jax import lax
from jax.experimental import pallas as pl
from jax.experimental.pallas import tpu as pltpu
from jax.sharding import PartitionSpec as P

STEPS = 4
PATCH_POINTS = 128
GROUPS = 1
LAG = 0
CHUNKS = 4
BLOCK = 256
MESH = pl.DeviceIdType.MESH
ORDERS = ((0, 1, 2), (1, 0, 2))


def log2(n):
    return n.bit_length() - 1


def split(x):
    hi = x.astype(jnp.bfloat16)
    return hi, (x - hi.astype(jnp.float32)).astype(jnp.bfloat16)


def dot(a, b, dims):
    return lax.dot_general(a, b, (dims, ((), ())), preferred_element_type=jnp.float32)


NN = ((1,), (0,))
NT = ((1,), (1,))


def kernel(
    n_rows, n_cols, p_ref, start_ref, decay_ref, escape_ref, nodepos_ref, power_ref,
    final_ref, temps_ref, hist_ref,
    p_hi, p_lo, spread, state, lhs, t_part, t_rx, t_full, d_part, d_rx, d_full,
    all_power, power_t, shares, h_part, h_rx, send_sem, recv_sem,
):
    r, q = lax.axis_index("rows"), lax.axis_index("cols")
    kr, kc = log2(n_rows), log2(n_cols)
    scen, states = start_ref.shape
    nodes = p_ref.shape[0]
    size = scen // GROUPS
    tiles = size // 8
    share = scen // n_cols
    positions = spread.shape[0]

    def bit(i, b):
        return (i // (1 << b)) % 2

    def flip(i, b):
        return i + (1 - 2 * bit(i, b)) * (1 << b)

    def row_peer(b):
        return (flip(r, b), q)

    def col_peer(b):
        return (r, flip(q, b))

    barrier = pltpu.get_barrier_semaphore()
    peers = [row_peer(b) for b in range(kr)] + [col_peer(b) for b in range(kc)]
    for peer in peers:
        pl.semaphore_signal(barrier, inc=1, device_id=peer, device_id_type=MESH)

    state[...] = start_ref[...]
    used = [0]
    copies = []

    def send(src, dst, peer):
        slot = used[0]
        used[0] += 1
        copy = pltpu.make_async_remote_copy(
            src_ref=src, dst_ref=dst, send_sem=send_sem.at[slot], recv_sem=recv_sem.at[slot],
            device_id=peer, device_id_type=MESH,
        )
        copy.start()
        copies.append(copy)
        return copy

    @pl.loop(0, nodes // BLOCK)
    def _(i):
        at = pl.ds(pl.multiple_of(i * BLOCK, BLOCK), BLOCK)
        hi, lo = split(p_ref[at, :])
        p_hi[at, :] = hi
        p_lo[at, :] = lo

    rows_iota = lax.broadcasted_iota(jnp.int32, (positions, nodes), 0)
    spread[...] = jnp.where(rows_iota == nodepos_ref[...], 1.0, 0.0).astype(jnp.bfloat16)
    pl.semaphore_wait(barrier, len(peers))

    ready = []

    def power_chain():
        all_power[pl.ds(r, 1)] = power_ref[...][None]
        for b in range(kr):
            block = pl.ds((r // (1 << b)) * (1 << b), 1 << b)
            copy = send(all_power.at[block], all_power.at[block], row_peer(b))
            yield
            copy.wait_recv()
        for k in range(STEPS):
            table = all_power[:, k].reshape(positions, scen).T
            hi, lo = split(table)
            power_t[k, 0] = hi
            power_t[k, 1] = lo
        ready.append(True)

    def history_chain():
        hi, lo = split(shares[...].reshape(STEPS * share, nodes))
        both = dot(spread[...], hi, NT) + dot(spread[...], lo, NT)
        h_part[...] = (both * (1.0 / PATCH_POINTS)).reshape(n_rows, 8, STEPS * share)
        start, length, at = 0, n_rows, 0
        for b in reversed(range(kr)):
            length //= 2
            keep = start + bit(r, b) * length
            away = start + (1 - bit(r, b)) * length
            copy = send(h_part.at[pl.ds(away, length)], h_rx.at[pl.ds(at, length)], row_peer(b))
            yield
            copy.wait_recv()
            kept = pl.ds(keep, length)
            h_part[kept] = h_part[kept] + h_rx[pl.ds(at, length)]
            start, at = keep, at + length
        hist_ref[...] = h_part[pl.ds(r, 1)][0]

    extra = []

    def together(parts):
        while parts:
            parts = [part for part in parts if next(part, parts) is not parts]
            if parts:
                yield

    def cols_chain(k, g, c):
        start, length, at = g * tiles, tiles, g * tiles
        for b in range(kc - 1):
            length //= 2
            keep = start + bit(q, b) * length
            away = start + (1 - bit(q, b)) * length
            copy = send(t_part.at[k, c, pl.ds(away, length)], t_rx.at[k, c, pl.ds(at, length)], col_peer(b))
            yield
            copy.wait_recv()
            kept = pl.ds(keep, length)
            t_part[k, c, kept] = t_part[k, c, kept] + t_rx[k, c, pl.ds(at, length)]
            start, at = keep, at + length
        kept = pl.ds(start, length)
        copy = send(t_part.at[k, c, kept], t_rx.at[k, c, pl.ds(at, length)], col_peer(kc - 1))
        yield
        copy.wait_recv()
        t_full[k, c, kept] = t_part[k, c, kept] + t_rx[k, c, pl.ds(at, length)]
        for b in reversed(range(kc - 1)):
            kept = pl.ds(start, length)
            copy = send(t_full.at[k, c, kept], t_full.at[k, c, kept], col_peer(b))
            yield
            copy.wait_recv()
            start, length = start - bit(q, b) * length, 2 * length

    def rows_chain(k, g, c):
        units = d_part.shape[2] // GROUPS
        order = ORDERS[(g + c) % 2] if kr == 3 else tuple(range(kr))
        start, length, at = g * units, units, g * units
        for b in order[:-1]:
            length //= 2
            keep = start + bit(r, b) * length
            away = start + (1 - bit(r, b)) * length
            copy = send(d_part.at[k, c, pl.ds(away, length)], d_rx.at[k, c, pl.ds(at, length)], row_peer(b))
            yield
            copy.wait_recv()
            kept = pl.ds(keep, length)
            d_part[k, c, kept] = d_part[k, c, kept] + d_rx[k, c, pl.ds(at, length)]
            start, at = keep, at + length
        kept = pl.ds(start, length)
        copy = send(d_part.at[k, c, kept], d_rx.at[k, c, pl.ds(at, length)], row_peer(order[-1]))
        yield
        copy.wait_recv()
        d_full[k, c, kept] = d_part[k, c, kept] + d_rx[k, c, pl.ds(at, length)]
        for b in reversed(order[:-1]):
            kept = pl.ds(start, length)
            copy = send(d_full.at[k, c, kept], d_full.at[k, c, kept], row_peer(b))
            yield
            copy.wait_recv()
            start, length = start - bit(r, b) * length, 2 * length

    def chain(g):
        mine = slice(g * size, (g + 1) * size)
        width = d_part.shape[-1]
        unit0 = g * (d_part.shape[2] // GROUPS)
        piece, strip = nodes // CHUNKS, states // CHUNKS

        def load_lhs():
            for c in range(0, states, BLOCK):
                hi, lo = split(state[mine, c : c + BLOCK])
                lhs[g, :size, c : c + BLOCK] = hi
                lhs[g, size:, c : c + BLOCK] = lo

        load_lhs()
        for k in range(STEPS):
            parts = []
            for c in range(CHUNKS):

                @pl.loop(0, piece // BLOCK)
                def _(i):
                    local = pl.ds(pl.multiple_of(i * BLOCK, BLOCK), BLOCK)
                    at = pl.ds(pl.multiple_of(c * piece + i * BLOCK, BLOCK), BLOCK)
                    two = dot(lhs[g], p_hi[at, :], NT)
                    out = two[:size] + two[size:] + dot(lhs[g, :size], p_lo[at, :], NT)
                    t_part[k, c, pl.ds(g * tiles, tiles), :, local] = out.reshape(tiles, 8, BLOCK)

                parts.append(cols_chain(k, g, c))
                next(parts[-1])
            yield
            yield from together(parts)

            if g == GROUPS - 1:
                for c in range(CHUNKS):
                    own = t_full[k, c, pl.ds(q * (share // 8), share // 8)].reshape(share, piece)
                    shares[k, :, c * piece : (c + 1) * piece] = own
                    if k == STEPS - 1:
                        temps_ref[:, c * piece : (c + 1) * piece] = own
                if k == STEPS - 1:
                    extra.append(history_chain())

            while not ready:
                yield

            for c in range(CHUNKS):

                @pl.loop(0, piece // BLOCK)
                def _(i):
                    local = pl.ds(pl.multiple_of(i * BLOCK, BLOCK), BLOCK)
                    at = pl.ds(pl.multiple_of(c * piece + i * BLOCK, BLOCK), BLOCK)
                    heat = dot(power_t[k, 0, mine], spread[:, at], NN) + dot(power_t[k, 1, mine], spread[:, at], NN)
                    temp = t_full[k, c, pl.ds(g * tiles, tiles), :, local].reshape(size, BLOCK)
                    hi, lo = split(heat + escape_ref[:, at] * (1.0 + jnp.tanh(2.0 * temp)))
                    lhs[g, :size, at] = hi
                    lhs[g, size:, at] = lo

            parts = []
            for c in range(CHUNKS):

                @pl.loop(0, strip // BLOCK)
                def _(i):
                    at = pl.ds(pl.multiple_of(c * strip + i * BLOCK, BLOCK), BLOCK)
                    two = dot(lhs[g], p_hi[:, at], NN)
                    out = two[:size] + two[size:] + dot(lhs[g, :size], p_lo[:, at], NN)
                    unit = (i * BLOCK) // width
                    inner = pl.ds(pl.multiple_of((i * BLOCK) % width, BLOCK), BLOCK)
                    d_part[k, c, pl.ds(unit0 + unit * tiles, tiles), :, inner] = out.reshape(tiles, 8, BLOCK)

                parts.append(rows_chain(k, g, c))
                next(parts[-1])
            yield
            yield from together(parts)

            for c in range(CHUNKS):
                for j in range(strip // width):
                    cols = slice(c * strip + j * width, c * strip + (j + 1) * width)
                    keep_share = decay_ref[:, cols]
                    driven = d_full[k, c, unit0 + j * tiles : unit0 + (j + 1) * tiles].reshape(size, width)
                    state[mine, cols] = keep_share * state[mine, cols] + (1.0 - keep_share) * driven
            if k < STEPS - 1:
                load_lhs()
            else:
                final_ref[mine, :] = state[mine, :]

    running = [(0, power_chain())] + [(g * LAG, chain(g)) for g in range(GROUPS)]
    tick = 0
    while running or extra:
        running += [(tick, c) for c in extra]
        extra.clear()
        left = []
        for when, c in running:
            if when > tick:
                left.append((when, c))
                continue
            try:
                next(c)
                left.append((when, c))
            except StopIteration:
                pass
        running = left
        tick += 1
    for copy in copies:
        copy.wait_send()


def shards(projector_matrix, start_state, decay_rate, escape_heat_factor, tile_block, block_owner, owner_power):
    n_rows, n_cols = lax.axis_size("rows"), lax.axis_size("cols")
    kr, kc = log2(n_rows), log2(n_cols)
    nodes, states = projector_matrix.shape
    scen = start_state.shape[0]
    share = scen // n_cols
    per_owner = owner_power.shape[2]
    blocks = block_owner.shape[0]
    ids = jnp.arange(blocks, dtype=jnp.int32)
    same = (block_owner[:, None] == block_owner[None, :]) & (ids[None, :] < ids[:, None])
    position = block_owner * per_owner + jnp.sum(same.astype(jnp.int32), axis=1)
    tile_position = jnp.sum(jnp.where(tile_block[:, None] == ids[None, :], position[None, :], 0), axis=1)
    node_position = jnp.repeat(tile_position, PATCH_POINTS)[None, :]
    size = scen // GROUPS
    tiles = size // 8
    need = n_rows // 2
    width = states // CHUNKS
    while (tiles * (states // CHUNKS // width)) % need:
        width //= 2
    units = GROUPS * tiles * (states // CHUNKS // width)
    sems = STEPS * GROUPS * CHUNKS * (2 * kr - 1 + 2 * kc - 1) + 2 * kr
    f32, b16 = jnp.float32, jnp.bfloat16
    vmem = pl.BlockSpec(memory_space=pltpu.VMEM)
    final, temps, hist = pl.pallas_call(
        functools.partial(kernel, n_rows, n_cols),
        out_shape=(
            jax.ShapeDtypeStruct((scen, states), f32),
            jax.ShapeDtypeStruct((share, nodes), f32),
            jax.ShapeDtypeStruct((per_owner, STEPS * share), f32),
        ),
        in_specs=[vmem] * 6,
        out_specs=(vmem,) * 3,
        scratch_shapes=[
            pltpu.VMEM((nodes, states), b16),
            pltpu.VMEM((nodes, states), b16),
            pltpu.VMEM((blocks, nodes), b16),
            pltpu.VMEM((scen, states), f32),
            pltpu.VMEM((GROUPS, 2 * size, max(states, nodes)), b16),
            pltpu.VMEM((STEPS, CHUNKS, scen // 8, 8, nodes // CHUNKS), f32),
            pltpu.VMEM((STEPS, CHUNKS, scen // 8, 8, nodes // CHUNKS), f32),
            pltpu.VMEM((STEPS, CHUNKS, scen // 8, 8, nodes // CHUNKS), f32),
            pltpu.VMEM((STEPS, CHUNKS, units, 8, width), f32),
            pltpu.VMEM((STEPS, CHUNKS, units, 8, width), f32),
            pltpu.VMEM((STEPS, CHUNKS, units, 8, width), f32),
            pltpu.VMEM((n_rows, STEPS, per_owner, scen), f32),
            pltpu.VMEM((STEPS, 2, scen, blocks), b16),
            pltpu.VMEM((STEPS, share, nodes), f32),
            pltpu.VMEM((n_rows, per_owner, STEPS * share), f32),
            pltpu.VMEM((n_rows, per_owner, STEPS * share), f32),
            pltpu.SemaphoreType.DMA((sems,)),
            pltpu.SemaphoreType.DMA((sems,)),
        ],
        compiler_params=pltpu.CompilerParams(
            collective_id=0, has_side_effects=True, vmem_limit_bytes=60 * 1024 * 1024
        ),
    )(
        projector_matrix, start_state, decay_rate[None, :], escape_heat_factor[None, :],
        node_position, jnp.transpose(owner_power, (0, 2, 1)),
    )
    history = jnp.transpose(hist.reshape(per_owner, STEPS, share), (1, 2, 0))
    return final, temps, history


def solution(mesh):
    placed = (
        P("rows", "cols"),
        P(None, "cols"),
        P("cols"),
        P("rows"),
        P("rows"),
        P(),
        P(None, None, "rows"),
    )
    return jax.shard_map(
        shards,
        mesh=mesh,
        in_specs=placed,
        out_specs=(P(None, "cols"), P("cols", "rows"), P(None, "cols", "rows")),
        check_vma=False,
    )
```
